512 devices in a mesh: group: 2 (over z_lo), dp: 8 (over y), tensor: 32 (over z_hi, x, core).
Axes of the slice: x: 4, y: 8, z: 8 (z_hi: 4, z_lo: 2; z = z_hi * 2 + z_lo), core: 2. Of those that a mesh axis runs over, the one named last changes fastest.
Arguments:
- image_feats: bfloat16 [2048, 7680], P('tensor', ('group', 'dp')), may hold values from -6 to 6
- proj_weight: bfloat16 [7680, 8192], P(('group', 'dp'), 'tensor'), may hold values from -0.0625 to 0.0625
- proj_bias: bfloat16 [8192], P('tensor'), may hold values from -3 to 3
- kv_weight: bfloat16 [8192, 2048], P('tensor'), may hold values from -0.0625 to 0.0625
- queries: bfloat16 [4096, 8192], P(('group', 'dp'), 'tensor'), may hold values from -14 to 14
- out_grad: bfloat16 [4096, 8192], P(('group', 'dp'), 'tensor'), may hold values from -6 to 6
- image_sample: int32 [16, 128], P(('group', 'dp')), may hold values from 0 to 3, as said below
- text_sample: int32 [16, 256], P(('group', 'dp')), may hold values from 0 to 3, as said below
Outputs:
- attended: bfloat16 [4096, 8192], P(('group', 'dp'), 'tensor')
- d_queries: bfloat16 [4096, 8192], P(('group', 'dp'), 'tensor')
- d_proj_weight: bfloat16 [7680, 8192], P(('group', 'dp'), 'tensor')
- d_proj_bias: float32 [8192], P('tensor')
- d_kv_weight: bfloat16 [8192, 2048], P('tensor', ('group', 'dp'))
The draws below stay inside these ranges and needn't reach their ends.
Inputs may be any that keep to these rules, and one draw needn't show every extreme that they name: `image_sample`: within each row (one data shard) the sample numbers never fall and every number from 0 to 3 occurs. `text_sample`: within each row (one data shard) the sample numbers never fall and every number from 0 to 3 occurs.
All inputs are finite; a program needn't handle non-finite values.
Results may differ from the reference program's by a relative error of at most 0.04.
Values may be sent and summed in bfloat16 or wider, within the bound.
A program may use at most 64 MiB of HBM per device.

```python
import jax
import jax.numpy as jnp
from jax import lax

VD = 7680
D = 8192
H = 64
KVH = 8
HD = 128
IMG_DEV = 128
TXT_DEV = 256
SAMPLES = 4
DATA = 16
IMAGE_ROWS = 2048
TEXT_ROWS = 4096
KV_COLS = 2048


def sample_numbers(key, length):
    jitter = max(1, length // (2 * SAMPLES))
    base = jnp.arange(1, SAMPLES, dtype=jnp.int32) * length // SAMPLES
    offsets = jax.random.randint(key, (DATA, SAMPLES - 1), 0, jitter + 1, dtype=jnp.int32)
    cuts = base[None, :] + offsets
    places = jnp.arange(length, dtype=jnp.int32)
    return jnp.sum((places[None, :, None] >= cuts[:, None, :]).astype(jnp.int32), axis=2)


def draw_image_sample(key, part):
    return sample_numbers(jax.random.fold_in(key, 11), IMG_DEV)


def draw_text_sample(key, part):
    return sample_numbers(jax.random.fold_in(key, 12), TXT_DEV)


def draw_queries(key, part):
    first = jax.random.fold_in(jax.random.fold_in(key, 13), 0)
    shape = (TEXT_ROWS, H * HD)
    values = jnp.clip(jax.random.normal(first, shape, jnp.float32), -6.0, 6.0)
    return values.astype(jnp.bfloat16)


def strengthened(values, own_key, source, target, blocks, factor):
    owner, partner = [(jnp.arange(values.shape[axis_at]) // (values.shape[axis_at] // blocks)).reshape([-1 if axis == axis_at else 1 for axis in range(values.ndim)]) for axis_at in (source, target)]
    chosen = jax.random.permutation(own_key, blocks)[partner]
    strong = (owner == chosen) | (owner == (partner + blocks // 2) % blocks)
    return jnp.where(strong, factor * values, values)


def level_of(rng, dims, cuts, smallest, top_value):
    gain, own = 1.0, jax.random.fold_in(rng, 6)
    for axis_at, parts in cuts:
        heights = jnp.exp(jax.random.uniform(jax.random.fold_in(own, axis_at), (parts,), jnp.float32, smallest / len(cuts), top_value / len(cuts)))
        gain = gain * jnp.repeat(heights, dims[axis_at] // parts).reshape([-1 if axis == axis_at else 1 for axis in range(len(dims))])
    return gain


def bell_draw(own_key, dims, width, limit, cuts=(), held_as=jnp.bfloat16):
    gain = level_of(own_key, dims, cuts, -0.22, 0.18) if cuts else 1.0
    values = jax.random.normal(own_key, dims, jnp.float32) * width * gain
    return jnp.minimum(jnp.maximum(values, -limit), limit).astype(held_as)


def gaussian_with(key, extent, scale, most, cuts, heavy, kind=jnp.bfloat16):
    values = scale * jax.random.normal(key, extent, jnp.float32)
    if cuts:
        values = values * level_of(key, extent, cuts, -0.22, 0.18)
    return jnp.clip(strengthened(values, jax.random.fold_in(key, 3), *heavy), -most, most).astype(kind)


def setup_inputs(seed: int = 0) -> dict:
    streams_of = jax.random.split(jax.random.key(seed), 9)
    return {
        "image_feats": gaussian_with(streams_of[0], (IMAGE_ROWS, VD), 1.0, 6.0, ((0, 32), (1, 16)), (1, 0, 32, 2.75)),
        "proj_weight": bell_draw(streams_of[1], (VD, D), VD ** -0.5, 0.0625, ((0, 16), (1, 32))),
        "proj_bias": bell_draw(streams_of[2], (D,), 0.5, 3.0, ((0, 32),)),
        "kv_weight": bell_draw(streams_of[3], (D, KV_COLS), D ** -0.5, 0.0625, ((0, 32),)),
        "queries": draw_queries(jax.random.fold_in(streams_of[8], 71), 0),
        "out_grad": bell_draw(streams_of[5], (TEXT_ROWS, H * HD), 1.0, 6.0, ((0, 16), (1, 32))),
        "image_sample": draw_image_sample(jax.random.fold_in(streams_of[8], 71), 0),
        "text_sample": draw_text_sample(jax.random.fold_in(streams_of[8], 71), 0),
    }


def shard_attention(q_rows, keys, values, grads, image_ids, text_ids):
    scale = HD ** -0.5
    qf = q_rows.astype(jnp.float32)
    kf = keys.astype(jnp.float32)
    vf = values.astype(jnp.float32)
    gf = grads.astype(jnp.float32)
    scores = jnp.einsum('thd,ihd->hti', qf, kf) * scale
    allowed = text_ids[:, None] == image_ids[None, :]
    scores = jnp.where(allowed[None], scores, jnp.float32(-1e30))
    peak = jnp.max(scores, axis=-1, keepdims=True)
    expo = jnp.exp(scores - peak)
    probs = expo / jnp.sum(expo, axis=-1, keepdims=True)
    probs_b = probs.astype(jnp.bfloat16)
    pf = probs_b.astype(jnp.float32)
    attended = jnp.einsum('hti,ihd->thd', pf, vf).astype(jnp.bfloat16)
    dprobs = jnp.einsum('thd,ihd->hti', gf, vf)
    delta = jnp.sum(probs * dprobs, axis=-1, keepdims=True)
    dscores = (probs * (dprobs - delta) * scale).astype(jnp.bfloat16)
    df = dscores.astype(jnp.float32)
    d_rows = jnp.einsum('hti,ihd->thd', df, kf).astype(jnp.bfloat16)
    d_keys = jnp.einsum('hti,thd->ihd', df, qf)
    d_values = jnp.einsum('hti,thd->ihd', pf, gf)
    return attended, d_rows, d_keys, d_values


def reference(image_feats, proj_weight, proj_bias, kv_weight, queries, out_grad, image_sample, text_sample):
    block = VD // DATA

    def add_block(total, index):
        feats = lax.dynamic_slice_in_dim(image_feats, index * block, block, 1)
        weight = lax.dynamic_slice_in_dim(proj_weight, index * block, block, 0)
        part = jnp.dot(feats, weight, preferred_element_type=jnp.float32).astype(jnp.bfloat16)
        return total + part.astype(jnp.float32), None

    summed, _ = lax.scan(add_block, jnp.zeros((IMAGE_ROWS, D), jnp.float32), jnp.arange(DATA, dtype=jnp.int32))
    projected = (summed + proj_bias.astype(jnp.float32)[None, :]).astype(jnp.bfloat16)
    kv = jnp.dot(projected, kv_weight, preferred_element_type=jnp.float32).astype(jnp.bfloat16)
    half = KVH * HD
    shared = H // KVH
    keys = jnp.repeat(kv[:, :half].reshape(DATA, IMG_DEV, KVH, HD), shared, axis=2)
    values = jnp.repeat(kv[:, half:].reshape(DATA, IMG_DEV, KVH, HD), shared, axis=2)
    q_rows = queries.reshape(DATA, TXT_DEV, H, HD)
    grads = out_grad.reshape(DATA, TXT_DEV, H, HD)

    def one_shard(items):
        return shard_attention(*items)

    attended, d_rows, d_keys, d_values = lax.map(one_shard, (q_rows, keys, values, grads, image_sample, text_sample))
    d_keys = jnp.sum(d_keys.reshape(DATA, IMG_DEV, KVH, shared, HD), axis=3).reshape(IMAGE_ROWS, half)
    d_values = jnp.sum(d_values.reshape(DATA, IMG_DEV, KVH, shared, HD), axis=3).reshape(IMAGE_ROWS, half)
    dkv = jnp.concatenate([d_keys, d_values], axis=1).astype(jnp.bfloat16)
    d_projected = jnp.dot(dkv, kv_weight.T, preferred_element_type=jnp.float32).astype(jnp.bfloat16)

    def add_shard(total, index):
        rows = lax.dynamic_slice_in_dim(projected, index * IMG_DEV, IMG_DEV, 0)
        grads_rows = lax.dynamic_slice_in_dim(dkv, index * IMG_DEV, IMG_DEV, 0)
        part = jnp.dot(rows.T, grads_rows, preferred_element_type=jnp.float32).astype(jnp.bfloat16)
        return total + part.astype(jnp.float32), None

    kv_total, _ = lax.scan(add_shard, jnp.zeros((D, KV_COLS), jnp.float32), jnp.arange(DATA, dtype=jnp.int32))
    d_kv_weight = kv_total.astype(jnp.bfloat16)
    d_proj_weight = jnp.dot(image_feats.T, d_projected, preferred_element_type=jnp.float32).astype(jnp.bfloat16)
    d_proj_bias = jnp.sum(d_projected.astype(jnp.float32), axis=0)
    attended = attended.reshape(TEXT_ROWS, H * HD)
    d_queries = d_rows.reshape(TEXT_ROWS, H * HD)
    return attended, d_queries, d_proj_weight, d_proj_bias, d_kv_weight
```

```python
import jax
import jax.numpy as jnp
from jax import lax
from jax.experimental import pallas as pl
from jax.experimental.pallas import tpu as pltpu
from jax.sharding import PartitionSpec as P

MESH = pl.DeviceIdType.MESH
BF = jnp.bfloat16
F32 = jnp.float32
HD = 128
KVH = 8
SCALE = HD ** (-0.5)


def dot(a, b, ca=1, cb=0):
    return lax.dot_general(a, b, (((ca,), (cb,)), ((), ())), preferred_element_type=F32)


class Names:
    def __init__(self):
        self.slots = {}

    def __getitem__(self, name):
        return self.slots.setdefault(name, len(self.slots))


SLOTS = 160


def kernel(
    feat_ref, w_ref, bias_ref, kvw_ref, q_ref, g_ref, img_ref, txt_ref,
    att_ref, dq_ref, dw_ref, db_ref, dkw_ref,
    F, FT, W, own, KT, sh, sw, rh, rw, zb, proj, projT, sh2, sw2, rh2, rw2, held, zs, zr_,
    kvp, kvr, sx, rx, sz, rz, kvg, dks, dkr, D, G, ssem, rsem,
):
    zl = lax.axis_index("group")
    y = lax.axis_index("dp")
    t = lax.axis_index("tensor")
    zh = t // 8
    x = (t // 2) % 4
    c = t % 2

    def T(zr=0, xr=0, cr=0):
        return ((zh + zr) % 4) * 8 + ((x + xr) % 4) * 2 + (c + cr) % 2

    xf = x + 1 - 2 * (x % 2)

    def TF(cr):
        return zh * 8 + xf * 2 + (c + cr) % 2

    zdev = {r: {"tensor": T(zr=r)} for r in (1, 2, 3)}
    xdev = {r: {"tensor": T(xr=r)} for r in (1, 2, 3)}
    core = {"tensor": T(cr=1)}
    ydev = {1: {"dp": (y + 1) % 8}, -1: {"dp": (y + 7) % 8}}
    twin = {"group": 1 - zl}
    flips = ({"tensor": T(cr=1)}, {"tensor": TF(0)}, {"tensor": TF(1)})

    names = Names()
    sends = []

    def send(src, dst, name, dev):
        k = names[name]
        copy = pltpu.make_async_remote_copy(
            src_ref=src, dst_ref=dst, send_sem=ssem.at[k], recv_sem=rsem.at[k],
            device_id=dev, device_id_type=MESH,
        )
        copy.start()
        sends.append(copy)

    def arrive(ref, name):
        k = names[name]
        pltpu.make_async_remote_copy(
            src_ref=ref, dst_ref=ref, send_sem=ssem.at[k], recv_sem=rsem.at[k],
            device_id=core, device_id_type=MESH,
        ).wait_recv()

    barrier = pltpu.get_barrier_semaphore()
    peers = [*zdev.values(), *xdev.values(), *ydev.values(), twin, core, flips[2]]
    for dev in peers:
        pl.semaphore_signal(barrier, inc=1, device_id=dev, device_id_type=MESH)

    own[...] = jnp.zeros_like(own)
    own[:, 0:480] = feat_ref[...]
    F[t] = own[...]
    W[480:512, :] = jnp.zeros((32, 256), BF)
    W[0:480, :] = w_ref[...]

    pl.semaphore_wait(barrier, len(peers))

    up, down = slice(0, 32), slice(32, 64)

    def spread(zr):
        ref = F.at[T(zr=zr)]
        send(ref, ref, f"x+{zr}", xdev[1])
        send(ref, ref, f"x-{zr}", xdev[3])

    def share(zr, xr):
        ref = F.at[T(zr, xr)]
        send(ref, ref, f"c{zr}{xr}", core)

    send(F.at[t], F.at[t], "z+", zdev[1])
    send(F.at[t], F.at[t], "z-", zdev[3])
    spread(0)
    share(0, 0)

    def bend(zr):
        for step, rows, to in ((3, up, 1), (1, down, 3)):
            ref = F.at[T(zr, step)]
            arrive(ref, f"x+{zr}" if step == 3 else f"x-{zr}")
            half = F.at[T(zr, step), rows]
            send(half, half, f"h{step}{zr}", xdev[to])
            share(zr, step)

    def last(zr):
        arrive(F.at[T(zr, 2), up], f"h3{zr}")
        arrive(F.at[T(zr, 2), down], f"h1{zr}")
        share(zr, 2)

    for h in range(KVH):
        for half in range(2):
            cols = pl.ds(half * 1024 + h * HD, HD)
            KT[h, pl.ds(half * HD, HD), :] = kvw_ref[:, cols].T

    arrive(F.at[T(3)], "z+")
    half = F.at[T(3), up]
    send(half, half, "zh3", zdev[1])
    spread(3)
    share(3, 0)
    arrive(F.at[T(1)], "z-")
    half = F.at[T(1), down]
    send(half, half, "zh1", zdev[3])
    spread(1)
    share(1, 0)
    bend(0)
    arrive(F.at[T(2), up], "zh3")
    arrive(F.at[T(2), down], "zh1")
    spread(2)
    share(2, 0)
    bend(3)
    bend(1)
    last(0)
    bend(2)
    last(3)
    last(1)
    last(2)
    for zr in range(4):
        for xr in range(4):
            arrive(F.at[T(zr, xr, 1)], f"c{zr}{xr}")

    def reduce_y(tag, tile, s_half, s_whole, r_half, r_whole, between=None):
        lanes = (slice(0, 128), slice(128, 256))
        for j in range(2):
            far = tile(j, (y + 4) % 8)
            for d, way in enumerate((1, -1)):
                s_half[d, j] = far[:, lanes[d]].astype(BF)
                send(s_half.at[d, j], r_half.at[d, j], f"{tag}{d}{j}0", ydev[way])
        for k in (1, 2, 3):
            if between is not None:
                between(k)
            for j in range(2):
                for d, way in enumerate((1, -1)):
                    part = tile(j, (y + way * (4 - k) + 8) % 8)
                    if k == 1:
                        arrive(r_half.at[d, j], f"{tag}{d}{j}0")
                        halves = [part[:, lanes[0]], part[:, lanes[1]]]
                        halves[d] = halves[d] + r_half[d, j].astype(F32)
                        for l in range(2):
                            s_whole[d, j, 0, :, lanes[l]] = halves[l].astype(BF)
                    else:
                        arrive(r_whole.at[d, j, k - 2], f"{tag}{d}{j}{k - 1}")
                        s_whole[d, j, k - 1] = (part + r_whole[d, j, k - 2].astype(F32)).astype(BF)
                    send(s_whole.at[d, j, k - 1], r_whole.at[d, j, k - 1], f"{tag}{d}{j}{k}", ydev[way])

    def settle_y(tag, j, tile, r_whole):
        total = tile(j, y)
        for d in range(2):
            arrive(r_whole.at[d, j, 2], f"{tag}{d}{j}3")
            total = total + r_whole[d, j, 2].astype(F32)
        return total

    def partial(j, row):
        shard = ((1 - zl if j == 0 else zl) * 8 + row) * 2
        rows = F[pl.ds(shard, 2)].reshape(128, 512)
        return dot(rows, W[...])

    reduce_y("p", partial, sh, sw, rh, rw)
    zb[0] = settle_y("p", 0, partial, rw).astype(BF)
    send(zb.at[0], zb.at[1], "pz", twin)
    total = settle_y("p", 1, partial, rw) + bias_ref[...].astype(F32)
    arrive(zb.at[1], "pz")
    projected = (total + zb[1].astype(F32)).astype(BF)
    proj[...] = projected

    for h in range(KVH):
        for half in range(2):
            cols = pl.ds(half * 1024 + h * HD, HD)
            block = dot(projected, kvw_ref[:, cols]).astype(BF)
            for m in range(4):
                kvp[m % 2, (h % 2) * 2 + m // 2, h // 2, :, pl.ds(half * HD, HD)] = block[32 * m : 32 * m + 32]
    send(kvp.at[1 - c], kvr, "kc", core)
    projT[...] = projected.T
    arrive(kvr, "kc")
    sx[...] = (kvp[c].astype(F32) + kvr[...].astype(F32)).astype(BF)
    for r in (2, 1, 3):
        send(sx.at[(x + r) % 4], rx.at[r - 1], f"kx{r}", xdev[r])

    def turn(lo, hi):
        def body(s, carry):
            rows = F[pl.ds(s * 2, 2)].reshape(128, 512)
            FT[:, pl.ds(pl.multiple_of(s * 128, 128), 128)] = rows.T
            return carry

        lax.fori_loop(lo, hi, body, 0)

    turn(0, 4)
    acc = sx[x].astype(F32)
    for r in (1, 3, 2):
        arrive(rx.at[r - 1], f"kx{r}")
        acc = acc + rx[r - 1].astype(F32)
    sz[...] = acc.astype(BF)
    for r in (2, 1, 3):
        send(sz.at[(zh + r) % 4], rz.at[r - 1], f"kz{r}", zdev[r])
    turn(4, 8)
    acc = sz[zh].astype(F32)
    for r in (1, 3, 2):
        arrive(rz.at[r - 1], f"kz{r}")
        acc = acc + rz[r - 1].astype(F32)
    m = (x % 2) * 2 + c
    kvg[m] = acc.astype(BF)
    for f, dev in enumerate(flips):
        send(kvg.at[m], kvg.at[m], f"kg{f}", dev)
    mates = ((x % 2) * 2 + 1 - c, (1 - x % 2) * 2 + c, (1 - x % 2) * 2 + 1 - c)
    for f in range(3):
        arrive(kvg.at[mates[f]], f"kg{f}")
    both = kvg[...].reshape(HD, 2 * HD)
    keys, values = both[:, :HD], both[:, HD:]

    allowed = txt_ref[...] == img_ref[...]
    dk = jnp.zeros((HD, HD), F32)
    dv = jnp.zeros((HD, HD), F32)
    for head in range(2):
        cols = slice(head * HD, head * HD + HD)
        q, g = q_ref[:, cols], g_ref[:, cols]
        scores = dot(q, keys, 1, 1) * SCALE
        scores = jnp.where(allowed, scores, F32(-1e30))
        expo = jnp.exp(scores - jnp.max(scores, axis=-1, keepdims=True))
        probs = expo / jnp.sum(expo, axis=-1, keepdims=True)
        probs_b = probs.astype(BF)
        att_ref[:, cols] = dot(probs_b, values).astype(BF)
        dprobs = dot(g, values, 1, 1)
        delta = jnp.sum(probs * dprobs, axis=-1, keepdims=True)
        dscores = (probs * (dprobs - delta) * SCALE).astype(BF)
        dq_ref[:, cols] = dot(dscores, keys).astype(BF)
        dk = dk + dot(dscores, q, 0, 0)
        dv = dv + dot(probs_b, g, 0, 0)

    stacked = jnp.concatenate([dk, dv], axis=1)
    dks[...] = stacked.reshape(4, 32, 2 * HD).astype(BF)
    for f, dev in enumerate(flips):
        send(dks.at[mates[f]], dkr.at[f], f"dk{f}", dev)
    mine = dks[m].astype(F32)
    for f in range(3):
        arrive(dkr.at[f], f"dk{f}")
        mine = mine + dkr[f].astype(F32)
    D[t] = mine.astype(BF)
    own_d = D.at[t]
    for r in (2, 1, 3):
        send(own_d, own_d, f"dz{r}", zdev[r])
    for r in (2, 1, 3):
        send(own_d, own_d, f"dx0{r}", xdev[r])
    send(own_d, own_d, "dc00", core)
    turn(8, 12)
    for r in (1, 3, 2):
        ref = D.at[T(4 - r)]
        arrive(ref, f"dz{r}")
        for s in (2, 1, 3):
            send(ref, ref, f"dx{4 - r}{s}", xdev[s])
        send(ref, ref, f"dc{4 - r}0", core)
    for zr in (0, 3, 1, 2):
        for s in (1, 3, 2):
            ref = D.at[T(zr, 4 - s)]
            arrive(ref, f"dx{zr}{s}")
            send(ref, ref, f"dc{zr}{4 - s}", core)
    for zr in range(4):
        for xr in range(4):
            arrive(D.at[T(zr, xr, 1)], f"dc{zr}{xr}")

    grad = jnp.zeros((128, 256), F32)
    for h in range(KVH):
        grad = grad + dot(D[4 * h : 4 * h + 4].reshape(128, 256), KT[h])

    def G_at(zr, yr):
        side = zl if zr == 0 else 1 - zl
        return G.at[side * 8 + (y + yr + 8) % 8]

    G[zl * 8 + y] = grad.astype(BF)
    piece = G_at(0, 0)
    send(piece, piece, "g+1", ydev[1])
    send(piece, piece, "g-1", ydev[-1])
    send(piece, piece, "gz0", twin)

    def weight_part(j, row):
        rows = D[pl.ds(row * 4, 4)].reshape(128, 256)
        return dot(projT[j * 128 : j * 128 + 128, :], rows)

    def pass_on(k):
        for way, sign, rows in ((1, "+", slice(0, 64)), (-1, "-", slice(64, 128))):
            piece = G_at(0, -way * k)
            arrive(piece, f"g{sign}{k}")
            if k < 3:
                send(piece, piece, f"g{sign}{k + 1}", ydev[way])
            else:
                index = zl * 8 + (y - way * k + 8) % 8
                send(G.at[index, rows], G.at[index, rows], f"g{sign}4", ydev[way])
            send(piece, piece, f"gz{sign}{k}", twin)

    reduce_y("w", weight_part, sh2, sw2, rh2, rw2, pass_on)
    turn(12, 16)
    opposite = zl * 8 + (y + 4) % 8
    arrive(G.at[opposite, slice(0, 64)], "g+4")
    arrive(G.at[opposite, slice(64, 128)], "g-4")
    send(G.at[opposite], G.at[opposite], "gz4", twin)
    mine_cols = pl.ds(pl.multiple_of(zl * 128, 128), 128)
    twin_cols = pl.ds(pl.multiple_of((1 - zl) * 128, 128), 128)
    for j in range(2):
        held[j] = settle_y("w", j, weight_part, rw2)
        zs[j] = held[j, :, twin_cols].astype(BF)
        send(zs.at[j], zr_.at[j], f"wz{j}", twin)

    def weight_grad(side):
        rows = G[pl.ds(side * 8, 8)].reshape(1024, 256)
        features = FT[:, pl.ds(pl.multiple_of(side * 1024, 1024), 1024)]
        return dot(features, rows), jnp.sum(rows.astype(F32), axis=0, keepdims=True)

    grad_w, grad_b = weight_grad(zl)
    for j in range(2):
        arrive(zr_.at[j], f"wz{j}")
        dkw_ref[j * 128 : j * 128 + 128, :] = (held[j, :, mine_cols] + zr_[j].astype(F32)).astype(BF)
    arrive(G_at(1, 0), "gz0")
    for k in (1, 2, 3):
        arrive(G_at(1, -k), f"gz+{k}")
        arrive(G_at(1, k), f"gz-{k}")
    arrive(G_at(1, 4), "gz4")
    more_w, more_b = weight_grad(1 - zl)
    dw_ref[...] = (grad_w + more_w)[0:480].astype(BF)
    db_ref[...] = grad_b + more_b
    for copy in sends:
        copy.wait_send()
    assert len(names.slots) <= SLOTS, len(names.slots)


def shards(
    image_feats, proj_weight, proj_bias, kv_weight, queries, out_grad, image_sample, text_sample
):
    vm = pltpu.VMEM
    out = pl.pallas_call(
        kernel,
        out_shape=(
            jax.ShapeDtypeStruct((256, 256), BF),
            jax.ShapeDtypeStruct((256, 256), BF),
            jax.ShapeDtypeStruct((480, 256), BF),
            jax.ShapeDtypeStruct((1, 256), F32),
            jax.ShapeDtypeStruct((256, 128), BF),
        ),
        in_specs=[pl.BlockSpec(memory_space=vm)] * 8,
        out_specs=[pl.BlockSpec(memory_space=vm)] * 5,
        scratch_shapes=[
            vm((32, 64, 512), BF),
            vm((512, 2048), BF),
            vm((512, 256), BF),
            vm((64, 512), BF),
            vm((KVH, 256, 256), BF),
            vm((2, 2, 128, 128), BF),
            vm((2, 2, 3, 128, 256), BF),
            vm((2, 2, 128, 128), BF),
            vm((2, 2, 3, 128, 256), BF),
            vm((2, 128, 256), BF),
            vm((128, 256), BF),
            vm((256, 128), BF),
            vm((2, 2, 128, 128), BF),
            vm((2, 2, 3, 128, 256), BF),
            vm((2, 2, 128, 128), BF),
            vm((2, 2, 3, 128, 256), BF),
            vm((2, 128, 256), F32),
            vm((2, 128, 128), BF),
            vm((2, 128, 128), BF),
            vm((2, 4, 4, 32, 256), BF),
            vm((4, 4, 32, 256), BF),
            vm((4, 4, 32, 256), BF),
            vm((3, 4, 32, 256), BF),
            vm((4, 32, 256), BF),
            vm((3, 32, 256), BF),
            vm((4, 32, 256), BF),
            vm((4, 32, 256), BF),
            vm((3, 32, 256), BF),
            vm((32, 32, 256), BF),
            vm((16, 128, 256), BF),
            pltpu.SemaphoreType.DMA((SLOTS,)),
            pltpu.SemaphoreType.DMA((SLOTS,)),
        ],
        compiler_params=pltpu.CompilerParams(
            collective_id=0, has_side_effects=True, vmem_limit_bytes=48 * 2**20
        ),
        name="layer",
    )(
        image_feats, proj_weight, proj_bias.reshape(1, 256), kv_weight, queries, out_grad,
        image_sample, text_sample.reshape(256, 1),
    )
    attended, d_queries, d_proj, d_bias, d_kv = out
    return attended, d_queries, d_proj, d_bias.reshape(256), d_kv


def solution(mesh):
    in_specs = (
        P("tensor", ("group", "dp")),
        P(("group", "dp"), "tensor"),
        P("tensor"),
        P("tensor", None),
        P(("group", "dp"), "tensor"),
        P(("group", "dp"), "tensor"),
        P(("group", "dp"), None),
        P(("group", "dp"), None),
    )
    out_specs = (
        P(("group", "dp"), "tensor"),
        P(("group", "dp"), "tensor"),
        P(("group", "dp"), "tensor"),
        P("tensor"),
        P("tensor", ("group", "dp")),
    )
    return jax.shard_map(shards, mesh=mesh, in_specs=in_specs, out_specs=out_specs, check_vma=False)
```

```python
import jax
import jax.numpy as jnp
from jax import lax
from jax.experimental import pallas as pl
from jax.experimental.pallas import tpu as pltpu
from jax.sharding import PartitionSpec as P

MESH = pl.DeviceIdType.MESH
BF = jnp.bfloat16
F32 = jnp.float32
HD = 128
KVH = 8
SCALE = HD ** (-0.5)


def dot(a, b, ca=1, cb=0):
    return lax.dot_general(a, b, (((ca,), (cb,)), ((), ())), preferred_element_type=F32)


class Names:
    def __init__(self):
        self.slots = {}

    def __getitem__(self, name):
        return self.slots.setdefault(name, len(self.slots))


SLOTS = 256
VMEM_ALL = 67043328
HALVES = (slice(0, 64), slice(64, 128))


def kernel(
    feat_in, w_in, bias_in, kvw_in, q_in, g_in, img_in, txt_in,
    att_out, dq_out, dw_out, db_out, dkw_out,
    F, FT, W, own, KT, sh, sw, rh, rw, zb, proj, projT, sh2, sw2, rh2, rw2, held, zs, zr_,
    kvp, kvr, sx, rx, sz, rz, kvg, dks, dkr, D, G,
    feat_ref, w_ref, bias_ref, kvw_ref, q_ref, g_ref, img_ref, txt_ref,
    att_ref, dq_ref, dw_ref, db_ref, dkw_ref, ssem, rsem, lsem,
):
    zl = lax.axis_index("group")
    y = lax.axis_index("dp")
    t = lax.axis_index("tensor")
    zh = t // 8
    x = (t // 2) % 4
    c = t % 2

    def T(zr=0, xr=0, cr=0):
        return ((zh + zr) % 4) * 8 + ((x + xr) % 4) * 2 + (c + cr) % 2

    xf = x + 1 - 2 * (x % 2)

    def TF(cr):
        return zh * 8 + xf * 2 + (c + cr) % 2

    zdev = {r: {"tensor": T(zr=r)} for r in (1, 2, 3)}
    xdev = {r: {"tensor": T(xr=r)} for r in (1, 2, 3)}
    core = {"tensor": T(cr=1)}
    ydev = {1: {"dp": (y + 1) % 8}, -1: {"dp": (y + 7) % 8}}
    twin = {"group": 1 - zl}
    flips = ({"tensor": T(cr=1)}, {"tensor": TF(0)}, {"tensor": TF(1)})

    names = Names()
    sends = []

    def send(src, dst, name, dev):
        k = names[name]
        copy = pltpu.make_async_remote_copy(
            src_ref=src, dst_ref=dst, send_sem=ssem.at[k], recv_sem=rsem.at[k],
            device_id=dev, device_id_type=MESH,
        )
        copy.start()
        sends.append(copy)

    def arrive(ref, name):
        k = names[name]
        pltpu.make_async_remote_copy(
            src_ref=ref, dst_ref=ref, send_sem=ssem.at[k], recv_sem=rsem.at[k],
            device_id=core, device_id_type=MESH,
        ).wait_recv()

    inputs = (feat_in, w_in, kvw_in, bias_in, q_in, g_in, img_in, txt_in)
    places = (feat_ref, w_ref, kvw_ref, bias_ref, q_ref, g_ref, img_ref, txt_ref)
    fetch = [pltpu.make_async_copy(a, b, lsem.at[i]) for i, (a, b) in enumerate(zip(inputs, places))]
    for copy in fetch:
        copy.start()

    barrier = pltpu.get_barrier_semaphore()
    peers = [*zdev.values(), *xdev.values(), *ydev.values(), twin, core, flips[2]]
    for dev in peers:
        pl.semaphore_signal(barrier, inc=1, device_id=dev, device_id_type=MESH)

    own[...] = jnp.zeros_like(own)
    fetch[0].wait()
    own[:, 0:480] = feat_ref[...]
    F[t] = own[...]

    pl.semaphore_wait(barrier, len(peers))

    def piece(zr, xr, half):
        return F.at[T(zr, xr), slice(32 * half, 32 * half + 32)]

    def spread(zr, half):
        ref = piece(zr, 0, half)
        send(ref, ref, f"x+{zr}{half}", xdev[1])
        send(ref, ref, f"x-{zr}{half}", xdev[3])

    def share(zr, xr):
        ref = F.at[T(zr, xr)]
        send(ref, ref, f"c{zr}{xr}", core)

    send(piece(0, 0, 0), piece(0, 0, 0), "z+0", zdev[1])
    send(piece(0, 0, 1), piece(0, 0, 1), "z-1", zdev[3])
    send(piece(0, 0, 0), piece(0, 0, 0), "x+00", xdev[1])
    send(piece(0, 0, 1), piece(0, 0, 1), "x-01", xdev[3])
    send(piece(0, 0, 1), piece(0, 0, 1), "z+1", zdev[1])
    send(piece(0, 0, 0), piece(0, 0, 0), "z-0", zdev[3])
    send(piece(0, 0, 1), piece(0, 0, 1), "x+01", xdev[1])
    send(piece(0, 0, 0), piece(0, 0, 0), "x-00", xdev[3])
    share(0, 0)
    for i in range(1, 8):
        fetch[i].wait()
    W[480:512, :] = jnp.zeros((32, 256), BF)
    W[0:480, :] = w_ref[...]

    def from_z(zr, half):
        ref = piece(zr, 0, half)
        if zr == 2:
            arrive(ref, f"zf{half}")
        else:
            arrive(ref, f"z+{half}" if zr == 3 else f"z-{half}")
            if (zr, half) == (3, 0):
                send(ref, ref, "zf0", zdev[1])
            if (zr, half) == (1, 1):
                send(ref, ref, "zf1", zdev[3])
        spread(zr, half)

    def from_x(zr, xr, half):
        ref = piece(zr, xr, half)
        arrive(ref, f"x+{zr}{half}" if xr == 3 else f"x-{zr}{half}")
        if (xr, half) == (3, 0):
            send(ref, ref, f"xf0{zr}", xdev[1])
        if (xr, half) == (1, 1):
            send(ref, ref, f"xf1{zr}", xdev[3])

    def last(zr):
        arrive(piece(zr, 2, 0), f"xf0{zr}")
        arrive(piece(zr, 2, 1), f"xf1{zr}")
        share(zr, 2)

    from_x(0, 3, 0)
    from_x(0, 1, 1)
    from_z(3, 0)
    from_z(1, 1)
    from_x(0, 3, 1)
    from_x(0, 1, 0)
    share(0, 3)
    share(0, 1)
    from_z(3, 1)
    from_z(1, 0)
    share(3, 0)
    share(1, 0)
    from_z(2, 0)
    from_z(2, 1)
    share(2, 0)
    from_x(3, 3, 0)
    from_x(1, 1, 1)
    from_x(3, 1, 0)
    from_x(1, 3, 1)
    from_x(3, 1, 1)
    from_x(1, 3, 0)
    from_x(3, 3, 1)
    from_x(1, 1, 0)
    for zr in (3, 1):
        share(zr, 3)
        share(zr, 1)
    last(0)
    from_x(2, 3, 0)
    from_x(2, 1, 1)
    from_x(2, 3, 1)
    from_x(2, 1, 0)
    share(2, 3)
    share(2, 1)
    last(3)
    last(1)
    last(2)
    for h in range(KVH):
        for half in range(2):
            cols = pl.ds(half * 1024 + h * HD, HD)
            KT[h, pl.ds(half * HD, HD), :] = kvw_ref[:, cols].T
    for zr in range(4):
        for xr in range(4):
            arrive(F.at[T(zr, xr, 1)], f"c{zr}{xr}")

    def reduce_y(tag, tile, s_half, s_whole, r_half, r_whole, between=None):
        lanes = (slice(0, 128), slice(128, 256))
        for j in range(2):
            far = tile(j, (y + 4) % 8)
            for n, rows in enumerate(HALVES):
                for d, way in enumerate((1, -1)):
                    s_half[d, j, rows, :] = far[rows, lanes[d]].astype(BF)
                    send(s_half.at[d, j, rows], r_half.at[d, j, rows], f"{tag}{d}{j}{n}0", ydev[way])
        for k in (1, 2, 3):
            if between is not None:
                between(k)
            for j in range(2):
                parts = [tile(j, (y + way * (4 - k) + 8) % 8) for way in (1, -1)]
                for n, rows in enumerate(HALVES):
                    for d, way in enumerate((1, -1)):
                        part = parts[d][rows]
                        if k == 1:
                            arrive(r_half.at[d, j, rows], f"{tag}{d}{j}{n}0")
                            halves = [part[:, lanes[0]], part[:, lanes[1]]]
                            halves[d] = halves[d] + r_half[d, j, rows, :].astype(F32)
                            for l in range(2):
                                s_whole[d, j, 0, rows, lanes[l]] = halves[l].astype(BF)
                        else:
                            got = r_whole.at[d, j, k - 2, rows]
                            arrive(got, f"{tag}{d}{j}{n}{k - 1}")
                            s_whole[d, j, k - 1, rows, :] = (part + got[...].astype(F32)).astype(BF)
                        source = s_whole.at[d, j, k - 1, rows]
                        send(source, r_whole.at[d, j, k - 1, rows], f"{tag}{d}{j}{n}{k}", ydev[way])

    def settle_y(tag, j, tile, r_whole, n):
        for d in range(2):
            got = r_whole.at[d, j, 2, HALVES[n]]
            arrive(got, f"{tag}{d}{j}{n}3")
            tile = tile + got[...].astype(F32)
        return tile

    def partial(j, row):
        shard = ((1 - zl if j == 0 else zl) * 8 + row) * 2
        rows = F[pl.ds(shard, 2)].reshape(128, 512)
        return dot(rows, W[...])

    reduce_y("p", partial, sh, sw, rh, rw)
    away = partial(0, y)
    home = partial(1, y) + bias_ref[...].astype(F32).reshape(1, 256)
    for n, rows in enumerate(HALVES):
        zb[0, rows, :] = settle_y("p", 0, away[rows], rw, n).astype(BF)
        send(zb.at[0, rows], zb.at[1, rows], f"pz{n}", twin)
    settled = [settle_y("p", 1, home[rows], rw, n) for n, rows in enumerate(HALVES)]
    for n, rows in enumerate(HALVES):
        arrive(zb.at[1, rows], f"pz{n}")
        settled[n] = settled[n] + zb[1, rows, :].astype(F32)
    projected = jnp.concatenate(settled, axis=0).astype(BF)
    proj[...] = projected

    for h in range(KVH):
        for half in range(2):
            cols = pl.ds(half * 1024 + h * HD, HD)
            block = dot(projected, kvw_ref[:, cols]).astype(BF)
            for m in range(4):
                kvp[m % 2, (h % 2) * 2 + m // 2, h // 2, :, pl.ds(half * HD, HD)] = block[32 * m : 32 * m + 32]
    send(kvp.at[1 - c], kvr, "kc", core)
    projT[...] = projected.T
    arrive(kvr, "kc")
    sx[...] = (kvp[c].astype(F32) + kvr[...].astype(F32)).astype(BF)
    for zr in (2, 1, 3, 0):
        for r in (2, 1, 3):
            send(sx.at[(x + r) % 4, (zh + zr) % 4], rx.at[r - 1, zr], f"kx{r}{zr}", xdev[r])

    def turn(lo, hi):
        def body(s, carry):
            rows = F[pl.ds(s * 2, 2)].reshape(128, 512)
            FT[:, pl.ds(pl.multiple_of(s * 128, 128), 128)] = rows.T
            return carry

        lax.fori_loop(lo, hi, body, 0)

    turn(0, 4)
    for zr in (2, 1, 3, 0):
        acc = sx[x, (zh + zr) % 4].astype(F32)
        for r in (1, 3, 2):
            arrive(rx.at[r - 1, zr], f"kx{r}{zr}")
            acc = acc + rx[r - 1, zr].astype(F32)
        if zr:
            sz[zr] = acc.astype(BF)
            send(sz.at[zr], rz.at[zr - 1], f"kz{zr}", zdev[zr])
    turn(4, 8)
    for r in (1, 3, 2):
        arrive(rz.at[r - 1], f"kz{r}")
        acc = acc + rz[r - 1].astype(F32)
    m = (x % 2) * 2 + c
    kvg[m] = acc.astype(BF)
    for f, dev in enumerate(flips):
        send(kvg.at[m], kvg.at[m], f"kg{f}", dev)
    texts = jnp.broadcast_to(txt_ref[...].astype(F32), (HD, 256)).T
    allowed = texts == img_ref[...].astype(F32)
    mates = ((x % 2) * 2 + 1 - c, (1 - x % 2) * 2 + c, (1 - x % 2) * 2 + 1 - c)
    for f in range(3):
        arrive(kvg.at[mates[f]], f"kg{f}")
    both = kvg[...].reshape(HD, 2 * HD)
    keys, values = both[:, :HD], both[:, HD:]

    dk = jnp.zeros((HD, HD), F32)
    dv = jnp.zeros((HD, HD), F32)
    for head in range(2):
        cols = slice(head * HD, head * HD + HD)
        q, g = q_ref[:, cols], g_ref[:, cols]
        scores = dot(q, keys, 1, 1) * SCALE
        scores = jnp.where(allowed, scores, F32(-1e30))
        expo = jnp.exp(scores - jnp.max(scores, axis=-1, keepdims=True))
        probs = expo / jnp.sum(expo, axis=-1, keepdims=True)
        probs_b = probs.astype(BF)
        att_ref[:, cols] = dot(probs_b, values).astype(BF)
        dprobs = dot(g, values, 1, 1)
        delta = jnp.sum(probs * dprobs, axis=-1, keepdims=True)
        dscores = (probs * (dprobs - delta) * SCALE).astype(BF)
        dq_ref[:, cols] = dot(dscores, keys).astype(BF)
        dk = dk + dot(dscores, q, 0, 0)
        dv = dv + dot(probs_b, g, 0, 0)

    stores = []

    def store(src, dst):
        copy = pltpu.make_async_copy(src, dst, lsem.at[8 + len(stores)])
        copy.start()
        stores.append(copy)

    store(att_ref, att_out)
    store(dq_ref, dq_out)

    stacked = jnp.concatenate([dk, dv], axis=1)
    dks[...] = stacked.reshape(4, 32, 2 * HD).astype(BF)
    for f, dev in enumerate(flips):
        send(dks.at[mates[f]], dkr.at[f], f"dk{f}", dev)
    mine = dks[m].astype(F32)
    for f in range(3):
        arrive(dkr.at[f], f"dk{f}")
        mine = mine + dkr[f].astype(F32)
    D[t] = mine.astype(BF)
    own_d = D.at[t]
    for r in (2, 1, 3):
        send(own_d, own_d, f"dz{r}", zdev[r])
    for r in (2, 1, 3):
        send(own_d, own_d, f"dx0{r}", xdev[r])
    send(own_d, own_d, "dc00", core)
    turn(8, 12)
    for r in (1, 3, 2):
        ref = D.at[T(4 - r)]
        arrive(ref, f"dz{r}")
        for s in (2, 1, 3):
            send(ref, ref, f"dx{4 - r}{s}", xdev[s])
        send(ref, ref, f"dc{4 - r}0", core)
    for zr in (0, 3, 1, 2):
        for s in (1, 3, 2):
            ref = D.at[T(zr, 4 - s)]
            arrive(ref, f"dx{zr}{s}")
            send(ref, ref, f"dc{zr}{4 - s}", core)
    for zr in range(4):
        for xr in range(4):
            arrive(D.at[T(zr, xr, 1)], f"dc{zr}{xr}")

    grad = jnp.zeros((128, 256), F32)
    for h in range(KVH):
        grad = grad + dot(D[4 * h : 4 * h + 4].reshape(128, 256), KT[h])

    def G_at(zr, yr):
        side = zl if zr == 0 else 1 - zl
        return G.at[side * 8 + (y + yr + 8) % 8]

    G[zl * 8 + y] = grad.astype(BF)
    piece = G_at(0, 0)
    send(piece, piece, "g+1", ydev[1])
    send(piece, piece, "g-1", ydev[-1])
    send(piece, piece, "gz0", twin)

    def weight_part(j, row):
        rows = D[pl.ds(row * 4, 4)].reshape(128, 256)
        return dot(projT[j * 128 : j * 128 + 128, :], rows)

    def pass_on(k):
        for way, sign, rows in ((1, "+", slice(0, 64)), (-1, "-", slice(64, 128))):
            piece = G_at(0, -way * k)
            arrive(piece, f"g{sign}{k}")
            if k < 3:
                send(piece, piece, f"g{sign}{k + 1}", ydev[way])
            else:
                index = zl * 8 + (y - way * k + 8) % 8
                send(G.at[index, rows], G.at[index, rows], f"g{sign}4", ydev[way])
            send(piece, piece, f"gz{sign}{k}", twin)

    reduce_y("w", weight_part, sh2, sw2, rh2, rw2, pass_on)
    turn(12, 16)
    opposite = zl * 8 + (y + 4) % 8
    for n, (rows, sign) in enumerate(zip(HALVES, "+-")):
        arrive(G.at[opposite, rows], f"g{sign}4")
        send(G.at[opposite, rows], G.at[opposite, rows], f"gz4{n}", twin)
    mine_cols = pl.ds(pl.multiple_of(zl * 128, 128), 128)
    twin_cols = pl.ds(pl.multiple_of((1 - zl) * 128, 128), 128)
    for j in range(2):
        near = weight_part(j, y)
        for n, rows in enumerate(HALVES):
            held[j, rows, :] = settle_y("w", j, near[rows], rw2, n)
        zs[j] = held[j, :, twin_cols].astype(BF)
        send(zs.at[j], zr_.at[j], f"wz{j}", twin)

    def weight_grad(side):
        rows = G[pl.ds(side * 8, 8)].reshape(1024, 256)
        features = FT[:, pl.ds(pl.multiple_of(side * 1024, 1024), 1024)]
        return dot(features, rows), jnp.sum(rows.astype(F32), axis=0, keepdims=True)

    grad_w, grad_b = weight_grad(zl)
    for j in range(2):
        arrive(zr_.at[j], f"wz{j}")
        dkw_ref[j * 128 : j * 128 + 128, :] = (held[j, :, mine_cols] + zr_[j].astype(F32)).astype(BF)
    store(dkw_ref, dkw_out)
    arrive(G_at(1, 0), "gz0")
    for k in (1, 2, 3):
        arrive(G_at(1, -k), f"gz+{k}")
        arrive(G_at(1, k), f"gz-{k}")
    for n, rows in enumerate(HALVES):
        arrive(G.at[(1 - zl) * 8 + (y + 4) % 8, rows], f"gz4{n}")
    more_w, more_b = weight_grad(1 - zl)
    dw_ref[...] = (grad_w + more_w)[0:480].astype(BF)
    db_ref[...] = grad_b + more_b
    store(dw_ref, dw_out)
    store(db_ref, db_out)
    for copy in sends:
        copy.wait_send()
    for copy in stores:
        copy.wait()
    assert len(names.slots) <= SLOTS, len(names.slots)


def write_out(*refs):
    given, result, held, sem = refs[:5], refs[5:10], refs[10:15], refs[15]
    load = [pltpu.make_async_copy(a, b, sem.at[i]) for i, (a, b) in enumerate(zip(given, held))]
    save = [pltpu.make_async_copy(a, b, sem.at[5 + i]) for i, (a, b) in enumerate(zip(held, result))]
    for copy in load:
        copy.start()
    for i in range(5):
        load[i].wait()
        save[i].start()
    for copy in save:
        copy.wait()


def shards(
    image_feats, proj_weight, proj_bias, kv_weight, queries, out_grad, image_sample, text_sample
):
    vm = pltpu.VMEM
    out = pl.pallas_call(
        kernel,
        out_shape=(
            jax.ShapeDtypeStruct((256, 256), BF),
            jax.ShapeDtypeStruct((256, 256), BF),
            jax.ShapeDtypeStruct((480, 256), BF),
            jax.ShapeDtypeStruct((1, 256), F32),
            jax.ShapeDtypeStruct((256, 128), BF),
        ),
        in_specs=[pl.BlockSpec(memory_space=pltpu.HBM)] * 8,
        out_specs=[pl.BlockSpec(memory_space=pltpu.HBM)] * 5,
        scratch_shapes=[
            vm((32, 64, 512), BF),
            vm((512, 2048), BF),
            vm((512, 256), BF),
            vm((64, 512), BF),
            vm((KVH, 256, 256), BF),
            vm((2, 2, 128, 128), BF),
            vm((2, 2, 3, 128, 256), BF),
            vm((2, 2, 128, 128), BF),
            vm((2, 2, 3, 128, 256), BF),
            vm((2, 128, 256), BF),
            vm((128, 256), BF),
            vm((256, 128), BF),
            vm((2, 2, 128, 128), BF),
            vm((2, 2, 3, 128, 256), BF),
            vm((2, 2, 128, 128), BF),
            vm((2, 2, 3, 128, 256), BF),
            vm((2, 128, 256), F32),
            vm((2, 128, 128), BF),
            vm((2, 128, 128), BF),
            vm((2, 4, 4, 32, 256), BF),
            vm((4, 4, 32, 256), BF),
            vm((4, 4, 32, 256), BF),
            vm((3, 4, 32, 256), BF),
            vm((4, 32, 256), BF),
            vm((3, 32, 256), BF),
            vm((4, 32, 256), BF),
            vm((4, 32, 256), BF),
            vm((3, 32, 256), BF),
            vm((32, 32, 256), BF),
            vm((16, 128, 256), BF),
            vm((64, 480), BF),
            vm((480, 256), BF),
            vm((256,), BF),
            vm((256, 2048), BF),
            vm((256, 256), BF),
            vm((256, 256), BF),
            vm((1, 128), jnp.int32),
            vm((1, 256), jnp.int32),
            vm((256, 256), BF),
            vm((256, 256), BF),
            vm((480, 256), BF),
            vm((1, 256), F32),
            vm((256, 128), BF),
            pltpu.SemaphoreType.DMA((SLOTS,)),
            pltpu.SemaphoreType.DMA((SLOTS,)),
            pltpu.SemaphoreType.DMA((13,)),
        ],
        compiler_params=pltpu.CompilerParams(
            collective_id=0, has_side_effects=True, vmem_limit_bytes=VMEM_ALL
        ),
        name="layer",
    )(
        image_feats, proj_weight, proj_bias, kv_weight, queries, out_grad,
        image_sample, text_sample,
    )
    out = pl.pallas_call(
        write_out,
        out_shape=[jax.ShapeDtypeStruct(a.shape, a.dtype) for a in out],
        in_specs=[pl.BlockSpec(memory_space=pltpu.HBM)] * 5,
        out_specs=[pl.BlockSpec(memory_space=pltpu.HBM)] * 5,
        scratch_shapes=[vm(a.shape, a.dtype) for a in out] + [pltpu.SemaphoreType.DMA((10,))],
        compiler_params=pltpu.CompilerParams(vmem_limit_bytes=VMEM_ALL),
        name="results",
    )(*out)
    attended, d_queries, d_proj, d_bias, d_kv = out
    return attended, d_queries, d_proj, d_bias.reshape(256), d_kv


def solution(mesh):
    in_specs = (
        P("tensor", ("group", "dp")),
        P(("group", "dp"), "tensor"),
        P("tensor"),
        P("tensor", None),
        P(("group", "dp"), "tensor"),
        P(("group", "dp"), "tensor"),
        P(("group", "dp"), None),
        P(("group", "dp"), None),
    )
    out_specs = (
        P(("group", "dp"), "tensor"),
        P(("group", "dp"), "tensor"),
        P(("group", "dp"), "tensor"),
        P("tensor"),
        P("tensor", ("group", "dp")),
    )
    return jax.shard_map(shards, mesh=mesh, in_specs=in_specs, out_specs=out_specs, check_vma=False)
```

```python
import jax
import jax.numpy as jnp
from jax import lax
from jax.experimental import pallas as pl
from jax.experimental.pallas import tpu as pltpu
from jax.sharding import PartitionSpec as P

MESH = pl.DeviceIdType.MESH
BF = jnp.bfloat16
F32 = jnp.float32
HD = 128
KVH = 8
SCALE = HD ** (-0.5)


def dot(a, b, ca=1, cb=0):
    return lax.dot_general(a, b, (((ca,), (cb,)), ((), ())), preferred_element_type=F32)


class Names:
    def __init__(self):
        self.slots = {}

    def __getitem__(self, name):
        return self.slots.setdefault(name, len(self.slots))


SLOTS = 256
VMEM_ALL = 67043328


def kernel(
    feat_in, w_in, bias_in, kvw_in, q_in, g_in, img_in, txt_in,
    att_out, dq_out, dw_out, db_out, dkw_out,
    F, FT, W, own, KT, sh, sw, rh, rw, zb, proj, projT, sh2, sw2, rh2, rw2, held, zs, zr_,
    kvp, kvr, sx, rx, sz, rz, kvg, dks, dkr, D, G,
    feat_ref, w_ref, bias_ref, kvw_ref, q_ref, g_ref, img_ref, txt_ref,
    att_ref, dq_ref, dw_ref, db_ref, dkw_ref, ssem, rsem, lsem,
):
    zl = lax.axis_index("group")
    y = lax.axis_index("dp")
    t = lax.axis_index("tensor")
    zh = t // 8
    x = (t // 2) % 4
    c = t % 2

    def T(zr=0, xr=0, cr=0):
        return ((zh + zr) % 4) * 8 + ((x + xr) % 4) * 2 + (c + cr) % 2

    xf = x + 1 - 2 * (x % 2)

    def TF(cr):
        return zh * 8 + xf * 2 + (c + cr) % 2

    zdev = {r: {"tensor": T(zr=r)} for r in (1, 2, 3)}
    xdev = {r: {"tensor": T(xr=r)} for r in (1, 2, 3)}
    core = {"tensor": T(cr=1)}
    ydev = {1: {"dp": (y + 1) % 8}, -1: {"dp": (y + 7) % 8}}
    twin = {"group": 1 - zl}
    flips = ({"tensor": T(cr=1)}, {"tensor": TF(0)}, {"tensor": TF(1)})

    names = Names()
    sends = []

    def send(src, dst, name, dev):
        k = names[name]
        copy = pltpu.make_async_remote_copy(
            src_ref=src, dst_ref=dst, send_sem=ssem.at[k], recv_sem=rsem.at[k],
            device_id=dev, device_id_type=MESH,
        )
        copy.start()
        sends.append(copy)

    def arrive(ref, name):
        k = names[name]
        pltpu.make_async_remote_copy(
            src_ref=ref, dst_ref=ref, send_sem=ssem.at[k], recv_sem=rsem.at[k],
            device_id=core, device_id_type=MESH,
        ).wait_recv()

    inputs = (feat_in, w_in, kvw_in, bias_in, q_in, g_in, img_in, txt_in)
    places = (feat_ref, w_ref, kvw_ref, bias_ref, q_ref, g_ref, img_ref, txt_ref)
    fetch = [pltpu.make_async_copy(a, b, lsem.at[i]) for i, (a, b) in enumerate(zip(inputs, places))]
    for copy in fetch:
        copy.start()

    barrier = pltpu.get_barrier_semaphore()
    peers = [*zdev.values(), *xdev.values(), *ydev.values(), twin, core, flips[2]]
    for dev in peers:
        pl.semaphore_signal(barrier, inc=1, device_id=dev, device_id_type=MESH)

    own[...] = jnp.zeros_like(own)
    fetch[0].wait()
    own[:, 0:480] = feat_ref[...]
    F[t] = own[...]

    pl.semaphore_wait(barrier, len(peers))

    def piece(zr, xr, half):
        return F.at[T(zr, xr), slice(32 * half, 32 * half + 32)]

    def spread(zr, half):
        ref = piece(zr, 0, half)
        send(ref, ref, f"x+{zr}{half}", xdev[1])
        send(ref, ref, f"x-{zr}{half}", xdev[3])

    def share(zr, xr):
        ref = F.at[T(zr, xr)]
        send(ref, ref, f"c{zr}{xr}", core)

    send(piece(0, 0, 0), piece(0, 0, 0), "z+0", zdev[1])
    send(piece(0, 0, 1), piece(0, 0, 1), "z-1", zdev[3])
    send(piece(0, 0, 0), piece(0, 0, 0), "x+00", xdev[1])
    send(piece(0, 0, 1), piece(0, 0, 1), "x-01", xdev[3])
    send(piece(0, 0, 1), piece(0, 0, 1), "z+1", zdev[1])
    send(piece(0, 0, 0), piece(0, 0, 0), "z-0", zdev[3])
    send(piece(0, 0, 1), piece(0, 0, 1), "x+01", xdev[1])
    send(piece(0, 0, 0), piece(0, 0, 0), "x-00", xdev[3])
    share(0, 0)
    for i in range(1, 8):
        fetch[i].wait()
    W[480:512, :] = jnp.zeros((32, 256), BF)
    W[0:480, :] = w_ref[...]

    def from_z(zr, half):
        ref = piece(zr, 0, half)
        if zr == 2:
            arrive(ref, f"zf{half}")
        else:
            arrive(ref, f"z+{half}" if zr == 3 else f"z-{half}")
            if (zr, half) == (3, 0):
                send(ref, ref, "zf0", zdev[1])
            if (zr, half) == (1, 1):
                send(ref, ref, "zf1", zdev[3])
        spread(zr, half)

    def from_x(zr, xr, half):
        ref = piece(zr, xr, half)
        arrive(ref, f"x+{zr}{half}" if xr == 3 else f"x-{zr}{half}")
        if (xr, half) == (3, 0):
            send(ref, ref, f"xf0{zr}", xdev[1])
        if (xr, half) == (1, 1):
            send(ref, ref, f"xf1{zr}", xdev[3])

    def last(zr):
        arrive(piece(zr, 2, 0), f"xf0{zr}")
        arrive(piece(zr, 2, 1), f"xf1{zr}")
        share(zr, 2)

    from_x(0, 3, 0)
    from_x(0, 1, 1)
    from_z(3, 0)
    from_z(1, 1)
    from_x(0, 3, 1)
    from_x(0, 1, 0)
    share(0, 3)
    share(0, 1)
    from_z(3, 1)
    from_z(1, 0)
    share(3, 0)
    share(1, 0)
    from_z(2, 0)
    from_z(2, 1)
    share(2, 0)
    from_x(3, 3, 0)
    from_x(1, 1, 1)
    from_x(3, 1, 0)
    from_x(1, 3, 1)
    from_x(3, 1, 1)
    from_x(1, 3, 0)
    from_x(3, 3, 1)
    from_x(1, 1, 0)
    for zr in (3, 1):
        share(zr, 3)
        share(zr, 1)
    last(0)
    from_x(2, 3, 0)
    from_x(2, 1, 1)
    from_x(2, 3, 1)
    from_x(2, 1, 0)
    share(2, 3)
    share(2, 1)
    last(3)
    last(1)
    last(2)

    def reduce_y(tag, tile, s_half, s_whole, r_half, r_whole, between):
        lanes = (slice(0, 128), slice(128, 256))
        for n in range(2):
            if n == 1:
                between(0)
            for j in range(2):
                far = tile(j, (y + 4) % 8, n)
                for d, way in enumerate((1, -1)):
                    s_half[d, j, n] = far[:, lanes[d]].astype(BF)
                    send(s_half.at[d, j, n], r_half.at[d, j, n], f"{tag}{d}{j}{n}0", ydev[way])
        for k in (1, 2, 3):
            between(k)
            for j in range(2):
                parts = [tile(j, (y + way * (4 - k) + 8) % 8, 2) for way in (1, -1)]
                for n in range(2):
                    for d, way in enumerate((1, -1)):
                        part = parts[d][64 * n : 64 * n + 64]
                        if k == 1:
                            arrive(r_half.at[d, j, n], f"{tag}{d}{j}{n}0")
                            halves = [part[:, lanes[0]], part[:, lanes[1]]]
                            halves[d] = halves[d] + r_half[d, j, n].astype(F32)
                            for l in range(2):
                                s_whole[d, j, n, 0, :, lanes[l]] = halves[l].astype(BF)
                        else:
                            arrive(r_whole.at[d, j, n, k - 2], f"{tag}{d}{j}{n}{k - 1}")
                            s_whole[d, j, n, k - 1] = (part + r_whole[d, j, n, k - 2].astype(F32)).astype(BF)
                        source = s_whole.at[d, j, n, k - 1]
                        send(source, r_whole.at[d, j, n, k - 1], f"{tag}{d}{j}{n}{k}", ydev[way])

    def settle_y(tag, j, total, r_whole, n):
        for d in range(2):
            arrive(r_whole.at[d, j, n, 2], f"{tag}{d}{j}{n}3")
            total = total + r_whole[d, j, n, 2].astype(F32)
        return total

    def partial(j, row, n):
        shard = ((1 - zl if j == 0 else zl) * 8 + row) * 2
        if n < 2:
            return dot(F[shard + (c + n) % 2], W[...])
        return dot(jnp.concatenate([F[shard + c], F[shard + 1 - c]], axis=0), W[...])

    def meanwhile(k):
        if k == 0:
            for zr in range(4):
                for xr in range(4):
                    arrive(F.at[T(zr, xr, 1)], f"c{zr}{xr}")
        if k == 1:
            for h in range(KVH):
                for half in range(2):
                    cols = pl.ds(half * 1024 + h * HD, HD)
                    KT[h, pl.ds(half * HD, HD), :] = kvw_ref[:, cols].T

    reduce_y("p", partial, sh, sw, rh, rw, meanwhile)
    both = partial(0, y, 2)
    away = [both[:64], both[64:]]
    both = partial(1, y, 2) + bias_ref[...].astype(F32).reshape(1, 256)
    home = [both[:64], both[64:]]
    for n in range(2):
        zb[0, n] = settle_y("p", 0, away[n], rw, n).astype(BF)
        send(zb.at[0, n], zb.at[1, n], f"pz{n}", twin)
        home[n] = settle_y("p", 1, home[n], rw, n)
    for n in range(2):
        arrive(zb.at[1, n], f"pz{n}")
        rows = pl.ds(pl.multiple_of((c + n) % 2 * 64, 64), 64)
        proj[rows, :] = (home[n] + zb[1, n].astype(F32)).astype(BF)
    projected = proj[...]

    for zr in (2, 1, 3, 0):
        zq = (zh + zr) % 4
        for half in range(2):
            cols = pl.ds(pl.multiple_of(half * 1024 + zq * 256, 256), 256)
            block = dot(projected, kvw_ref[:, cols]).astype(BF)
            for h in range(2):
                for m in range(4):
                    kvp[m // 2, zr, h * 2 + m % 2, :, pl.ds(half * HD, HD)] = block[
                        32 * m : 32 * m + 32, h * HD : h * HD + HD
                    ]
        send(kvp.at[1 - c, zr], kvr.at[zr], f"kc{zr}", core)
    for zr in (2, 1, 3, 0):
        arrive(kvr.at[zr], f"kc{zr}")
        sx[zr] = (kvp[c, zr].astype(F32) + kvr[zr].astype(F32)).astype(BF)
        for r in (2, 1, 3):
            send(sx.at[zr, (x + r) % 4], rx.at[r - 1, zr], f"kx{r}{zr}", xdev[r])
    projT[...] = projected.T

    def turn(lo, hi):
        def body(s, carry):
            rows = F[pl.ds(s * 2, 2)].reshape(128, 512)
            FT[:, pl.ds(pl.multiple_of(s * 128, 128), 128)] = rows.T
            return carry

        lax.fori_loop(lo, hi, body, 0)

    turn(0, 4)
    for zr in (2, 1, 3, 0):
        acc = sx[zr, x].astype(F32)
        for r in (1, 3, 2):
            arrive(rx.at[r - 1, zr], f"kx{r}{zr}")
            acc = acc + rx[r - 1, zr].astype(F32)
        if zr:
            sz[zr] = acc.astype(BF)
            send(sz.at[zr], rz.at[zr - 1], f"kz{zr}", zdev[zr])
    turn(4, 8)
    for r in (1, 3, 2):
        arrive(rz.at[r - 1], f"kz{r}")
        acc = acc + rz[r - 1].astype(F32)
    m = c * 2 + x % 2
    kvg[m] = acc.astype(BF)
    for f, dev in enumerate(flips):
        send(kvg.at[m], kvg.at[m], f"kg{f}", dev)
    texts = jnp.broadcast_to(txt_ref[...].astype(F32), (HD, 256)).T
    allowed = texts == img_ref[...].astype(F32)
    mates = (2 - 2 * c + x % 2, 2 * c + 1 - x % 2, 2 - 2 * c + 1 - x % 2)
    for f in range(3):
        arrive(kvg.at[mates[f]], f"kg{f}")
    both = kvg[...].reshape(HD, 2 * HD)
    keys, values = both[:, :HD], both[:, HD:]

    dk = jnp.zeros((HD, HD), F32)
    dv = jnp.zeros((HD, HD), F32)
    for head in range(2):
        cols = slice(head * HD, head * HD + HD)
        q, g = q_ref[:, cols], g_ref[:, cols]
        scores = dot(q, keys, 1, 1) * SCALE
        scores = jnp.where(allowed, scores, F32(-1e30))
        expo = jnp.exp(scores - jnp.max(scores, axis=-1, keepdims=True))
        probs = expo / jnp.sum(expo, axis=-1, keepdims=True)
        probs_b = probs.astype(BF)
        att_ref[:, cols] = dot(probs_b, values).astype(BF)
        dprobs = dot(g, values, 1, 1)
        delta = jnp.sum(probs * dprobs, axis=-1, keepdims=True)
        dscores = (probs * (dprobs - delta) * SCALE).astype(BF)
        dq_ref[:, cols] = dot(dscores, keys).astype(BF)
        dk = dk + dot(dscores, q, 0, 0)
        dv = dv + dot(probs_b, g, 0, 0)

    stores = []

    def store(src, dst):
        copy = pltpu.make_async_copy(src, dst, lsem.at[8 + len(stores)])
        copy.start()
        stores.append(copy)

    store(att_ref, att_out)
    store(dq_ref, dq_out)

    stacked = jnp.concatenate([dk, dv], axis=1)
    dks[...] = stacked.reshape(4, 32, 2 * HD).astype(BF)
    for f, dev in enumerate(flips):
        send(dks.at[mates[f]], dkr.at[f], f"dk{f}", dev)
    mine = dks[m].astype(F32)
    for f in range(3):
        arrive(dkr.at[f], f"dk{f}")
        mine = mine + dkr[f].astype(F32)

    def D_at(zr, xr, cr=0):
        xq = (x + xr) % 4
        return D.at[(((zh + zr) % 4 * 2 + xq // 2) * 2 + (c + cr) % 2) * 2 + xq % 2]

    own_d = D_at(0, 0)
    own_d[...] = mine.astype(BF)
    for r in (2, 1, 3):
        send(own_d, own_d, f"dz{r}", zdev[r])
    for r in (2, 1, 3):
        send(own_d, own_d, f"dx0{r}", xdev[r])
    send(own_d, own_d, "dc00", core)
    turn(8, 12)
    for r in (1, 3, 2):
        ref = D_at(4 - r, 0)
        arrive(ref, f"dz{r}")
        for s in (2, 1, 3):
            send(ref, ref, f"dx{4 - r}{s}", xdev[s])
        send(ref, ref, f"dc{4 - r}0", core)
    for zr in (0, 3, 1, 2):
        for s in (1, 3, 2):
            ref = D_at(zr, 4 - s)
            arrive(ref, f"dx{zr}{s}")
            send(ref, ref, f"dc{zr}{4 - s}", core)

    def G_at(zr, yr, n):
        side = zl if zr == 0 else 1 - zl
        return G.at[side * 8 + (y + yr + 8) % 8, (c + n) % 2]

    for n in range(2):
        if n == 1:
            for zr in range(4):
                for xr in range(4):
                    arrive(D_at(zr, xr, 1), f"dc{zr}{xr}")
        grad = jnp.zeros((64, 256), F32)
        for h in range(KVH):
            rows = D[pl.ds(4 * h + (c + n) % 2 * 2, 2)].reshape(64, 256)
            grad = grad + dot(rows, KT[h])
        piece = G_at(0, 0, n)
        piece[...] = grad.astype(BF)
        send(piece, piece, f"g+1{n}", ydev[1])
        send(piece, piece, f"g-1{n}", ydev[-1])
        send(piece, piece, f"gz0{n}", twin)

    def weight_part(j, row, n):
        rows = D[pl.ds(row * 4, 4)].reshape(128, 256)
        top = j * 128 + n % 2 * 64
        return dot(projT[top : top + (64 if n < 2 else 128), :], rows)

    def pass_on(k):
        if k == 0:
            return
        for n in range(2):
            for d, (way, sign) in enumerate(((1, "+"), (-1, "-"))):
                piece = G_at(0, -way * k, n)
                arrive(piece, f"g{sign}{k}{n}")
                if k < 3 or n == d:
                    send(piece, piece, f"g{sign}{k + 1}{n}", ydev[way])
                send(piece, piece, f"gz{sign}{k}{n}", twin)

    reduce_y("w", weight_part, sh2, sw2, rh2, rw2, pass_on)
    turn(12, 16)
    for n, sign in enumerate("+-"):
        piece = G_at(0, 4, n)
        arrive(piece, f"g{sign}4{n}")
        send(piece, piece, f"gz4{n}", twin)
    mine_cols = pl.ds(pl.multiple_of(zl * 128, 128), 128)
    twin_cols = pl.ds(pl.multiple_of((1 - zl) * 128, 128), 128)
    for j in range(2):
        near = weight_part(j, y, 2)
        for n in range(2):
            held[j, n] = settle_y("w", j, near[64 * n : 64 * n + 64], rw2, n)
            zs[j, n] = held[j, n, :, twin_cols].astype(BF)
            send(zs.at[j, n], zr_.at[j, n], f"wz{j}{n}", twin)

    def weight_grad(side):
        rows = G[pl.ds(side * 8, 8)].reshape(1024, 256)
        features = FT[:, pl.ds(pl.multiple_of(side * 1024, 1024), 1024)]
        return dot(features, rows), jnp.sum(rows.astype(F32), axis=0, keepdims=True)

    grad_w, grad_b = weight_grad(zl)
    for j in range(2):
        for n in range(2):
            arrive(zr_.at[j, n], f"wz{j}{n}")
            top = j * 128 + n * 64
            dkw_ref[top : top + 64, :] = (held[j, n, :, mine_cols] + zr_[j, n].astype(F32)).astype(BF)
    store(dkw_ref, dkw_out)
    for n in range(2):
        arrive(G_at(1, 0, n), f"gz0{n}")
        for k in (1, 2, 3):
            arrive(G_at(1, -k, n), f"gz+{k}{n}")
            arrive(G_at(1, k, n), f"gz-{k}{n}")
        arrive(G_at(1, 4, n), f"gz4{n}")
    more_w, more_b = weight_grad(1 - zl)
    dw_ref[...] = (grad_w + more_w)[0:480].astype(BF)
    db_ref[...] = grad_b + more_b
    store(dw_ref, dw_out)
    store(db_ref, db_out)
    for copy in sends:
        copy.wait_send()
    for copy in stores:
        copy.wait()
    assert len(names.slots) <= SLOTS, len(names.slots)


def write_out(*refs):
    given, result, held, sem = refs[:5], refs[5:10], refs[10:15], refs[15]
    load = [pltpu.make_async_copy(a, b, sem.at[i]) for i, (a, b) in enumerate(zip(given, held))]
    save = [pltpu.make_async_copy(a, b, sem.at[5 + i]) for i, (a, b) in enumerate(zip(held, result))]
    for copy in load:
        copy.start()
    for i in range(5):
        load[i].wait()
        save[i].start()
    for copy in save:
        copy.wait()


def shards(
    image_feats, proj_weight, proj_bias, kv_weight, queries, out_grad, image_sample, text_sample
):
    vm = pltpu.VMEM
    out = pl.pallas_call(
        kernel,
        out_shape=(
            jax.ShapeDtypeStruct((256, 256), BF),
            jax.ShapeDtypeStruct((256, 256), BF),
            jax.ShapeDtypeStruct((480, 256), BF),
            jax.ShapeDtypeStruct((1, 256), F32),
            jax.ShapeDtypeStruct((256, 128), BF),
        ),
        in_specs=[pl.BlockSpec(memory_space=pltpu.HBM)] * 8,
        out_specs=[pl.BlockSpec(memory_space=pltpu.HBM)] * 5,
        scratch_shapes=[
            vm((32, 64, 512), BF),
            vm((512, 2048), BF),
            vm((512, 256), BF),
            vm((64, 512), BF),
            vm((KVH, 256, 256), BF),
            vm((2, 2, 2, 64, 128), BF),
            vm((2, 2, 2, 3, 64, 256), BF),
            vm((2, 2, 2, 64, 128), BF),
            vm((2, 2, 2, 3, 64, 256), BF),
            vm((2, 2, 64, 256), BF),
            vm((128, 256), BF),
            vm((256, 128), BF),
            vm((2, 2, 2, 64, 128), BF),
            vm((2, 2, 2, 3, 64, 256), BF),
            vm((2, 2, 2, 64, 128), BF),
            vm((2, 2, 2, 3, 64, 256), BF),
            vm((2, 2, 64, 256), F32),
            vm((2, 2, 64, 128), BF),
            vm((2, 2, 64, 128), BF),
            vm((2, 4, 4, 32, 256), BF),
            vm((4, 4, 32, 256), BF),
            vm((4, 4, 32, 256), BF),
            vm((3, 4, 32, 256), BF),
            vm((4, 32, 256), BF),
            vm((3, 32, 256), BF),
            vm((4, 32, 256), BF),
            vm((4, 32, 256), BF),
            vm((3, 32, 256), BF),
            vm((32, 32, 256), BF),
            vm((16, 2, 64, 256), BF),
            vm((64, 480), BF),
            vm((480, 256), BF),
            vm((256,), BF),
            vm((256, 2048), BF),
            vm((256, 256), BF),
            vm((256, 256), BF),
            vm((1, 128), jnp.int32),
            vm((1, 256), jnp.int32),
            vm((256, 256), BF),
            vm((256, 256), BF),
            vm((480, 256), BF),
            vm((1, 256), F32),
            vm((256, 128), BF),
            pltpu.SemaphoreType.DMA((SLOTS,)),
            pltpu.SemaphoreType.DMA((SLOTS,)),
            pltpu.SemaphoreType.DMA((13,)),
        ],
        compiler_params=pltpu.CompilerParams(
            collective_id=0, has_side_effects=True, vmem_limit_bytes=VMEM_ALL
        ),
        name="layer",
    )(
        image_feats, proj_weight, proj_bias, kv_weight, queries, out_grad,
        image_sample, text_sample,
    )
    out = pl.pallas_call(
        write_out,
        out_shape=[jax.ShapeDtypeStruct(a.shape, a.dtype) for a in out],
        in_specs=[pl.BlockSpec(memory_space=pltpu.HBM)] * 5,
        out_specs=[pl.BlockSpec(memory_space=pltpu.HBM)] * 5,
        scratch_shapes=[vm(a.shape, a.dtype) for a in out] + [pltpu.SemaphoreType.DMA((10,))],
        compiler_params=pltpu.CompilerParams(vmem_limit_bytes=VMEM_ALL),
        name="results",
    )(*out)
    attended, d_queries, d_proj, d_bias, d_kv = out
    return attended, d_queries, d_proj, d_bias.reshape(256), d_kv


def solution(mesh):
    in_specs = (
        P("tensor", ("group", "dp")),
        P(("group", "dp"), "tensor"),
        P("tensor"),
        P("tensor", None),
        P(("group", "dp"), "tensor"),
        P(("group", "dp"), "tensor"),
        P(("group", "dp"), None),
        P(("group", "dp"), None),
    )
    out_specs = (
        P(("group", "dp"), "tensor"),
        P(("group", "dp"), "tensor"),
        P(("group", "dp"), "tensor"),
        P("tensor"),
        P("tensor", ("group", "dp")),
    )
    return jax.shard_map(shards, mesh=mesh, in_specs=in_specs, out_specs=out_specs, check_vma=False)
```
